16 devices in a mesh: fsdp: 16 (over z, y, x, core).
Axes of the slice: x: 2, y: 2, z: 2, core: 2. Of those that a mesh axis runs over, the one named last changes fastest.
Arguments:
- patches: bfloat16 [128, 256, 588], P('fsdp')
- keep: int32 [128, 128], P('fsdp')
- w_patch: float32 [588, 1024], P(None, 'fsdp')
- b_patch: float32 [1024], P('fsdp')
- pos_table: float32 [257, 1024], P(None, 'fsdp')
- cls_tok: float32 [1024], P('fsdp')
- lnp_g: float32 [1024], P('fsdp')
- lnp_b: float32 [1024], P('fsdp')
- ln1_g: float32 [1024], P('fsdp')
- ln1_b: float32 [1024], P('fsdp')
- w_qkv: float32 [1024, 3, 16, 64], P('fsdp')
- b_qkv: float32 [3072], P('fsdp')
- w_out: float32 [1024, 1024], P('fsdp')
- b_out: float32 [1024], P('fsdp')
- ln2_g: float32 [1024], P('fsdp')
- ln2_b: float32 [1024], P('fsdp')
- w_fc: float32 [1024, 4096], P('fsdp')
- b_fc: float32 [4096], P('fsdp')
- w_proj: float32 [4096, 1024], P('fsdp')
- b_proj: float32 [1024], P('fsdp')
- grad_h1: bfloat16 [128, 129, 1024], P('fsdp')
Outputs:
- output 1: bfloat16 [128, 129, 1024], P('fsdp')
- output 2: float32 [588, 1024], P(None, 'fsdp')
- output 3: float32 [1024], P('fsdp')
- output 4: float32 [257, 1024], P(None, 'fsdp')
- output 5: float32 [1024], P('fsdp')
- output 6: float32 [1024], P('fsdp')
- output 7: float32 [1024], P('fsdp')
- output 8: float32 [1024], P('fsdp')
- output 9: float32 [1024], P('fsdp')
- output 10: float32 [1024, 3, 16, 64], P('fsdp')
- output 11: float32 [3072], P('fsdp')
- output 12: float32 [1024, 1024], P('fsdp')
- output 13: float32 [1024], P('fsdp')
- output 14: float32 [1024], P('fsdp')
- output 15: float32 [1024], P('fsdp')
- output 16: float32 [1024, 4096], P('fsdp')
- output 17: float32 [4096], P('fsdp')
- output 18: float32 [4096, 1024], P('fsdp')
- output 19: float32 [1024], P('fsdp')
All inputs are finite; a program needn't handle non-finite values.
Results may differ from the reference program's by a relative error of at most 0.02.
Values are sent between devices in bfloat16 or wider.
A program may use at most 1 GiB of HBM per device.

```python
import jax
import jax.numpy as jnp
from jax import lax

MODEL_WIDTH = 1024
NUM_HEADS = 16
MLP_WIDTH = 4096
NUM_PATCHES = 256
PATCH_PIXELS = 588
NUM_KEEP = 128
BATCH_SIZE = 128
BLOCK_IMAGES = 8
TOKENS = NUM_KEEP + 1
HEAD_DIM = MODEL_WIDTH // NUM_HEADS
LN_EPS = 1e-5
INV_SQRT2 = 0.7071067811865476
INV_SQRT_2PI = 0.3989422804014327
PARAM_NAMES = ('w_patch', 'b_patch', 'pos_table', 'cls_tok', 'lnp_g', 'lnp_b', 'ln1_g', 'ln1_b', 'w_qkv', 'b_qkv', 'w_out', 'b_out', 'ln2_g', 'ln2_b', 'w_fc', 'b_fc', 'w_proj', 'b_proj')
VECTOR_NAMES = ('b_patch', 'cls_tok', 'lnp_g', 'lnp_b', 'ln1_g', 'ln1_b', 'b_qkv', 'b_out', 'ln2_g', 'ln2_b', 'b_fc', 'b_proj')


def setup_inputs(seed: int = 0) -> dict:
    key_list = jax.random.split(jax.random.key(seed), 21)
    d_model = MODEL_WIDTH
    mlp_width = MLP_WIDTH

    def draw_normal(index, shape, scale):
        return jax.random.normal(key_list[index], shape, jnp.float32) * scale

    def gain_vec(index):
        return 1.0 + draw_normal(index, (d_model,), 0.2)

    row_keys = jax.random.split(key_list[1], BATCH_SIZE)
    perm_rows = jax.vmap(lambda row_key: jax.random.permutation(row_key, NUM_PATCHES))(row_keys)
    return {
        'patches': draw_normal(0, (BATCH_SIZE, NUM_PATCHES, PATCH_PIXELS), 1.0).astype(jnp.bfloat16),
        'keep': perm_rows[:, :NUM_KEEP].astype(jnp.int32),
        'w_patch': draw_normal(2, (PATCH_PIXELS, d_model), PATCH_PIXELS ** -0.5),
        'b_patch': draw_normal(3, (d_model,), 0.3),
        'pos_table': draw_normal(4, (NUM_PATCHES + 1, d_model), 0.5),
        'cls_tok': draw_normal(5, (d_model,), 1.0),
        'lnp_g': gain_vec(6),
        'lnp_b': draw_normal(7, (d_model,), 0.2),
        'ln1_g': gain_vec(8),
        'ln1_b': draw_normal(9, (d_model,), 0.2),
        'w_qkv': draw_normal(10, (d_model, 3, NUM_HEADS, HEAD_DIM), d_model ** -0.5),
        'b_qkv': draw_normal(11, (3 * d_model,), 0.3),
        'w_out': draw_normal(12, (d_model, d_model), d_model ** -0.5),
        'b_out': draw_normal(13, (d_model,), 0.3),
        'ln2_g': gain_vec(14),
        'ln2_b': draw_normal(15, (d_model,), 0.2),
        'w_fc': draw_normal(16, (d_model, mlp_width), d_model ** -0.5),
        'b_fc': draw_normal(17, (mlp_width,), 0.3),
        'w_proj': draw_normal(18, (mlp_width, d_model), mlp_width ** -0.5),
        'b_proj': draw_normal(19, (d_model,), 0.3),
        'grad_h1': draw_normal(20, (BATCH_SIZE, TOKENS, d_model), (BATCH_SIZE * TOKENS) ** -0.5).astype(jnp.bfloat16),
    }


def product(einsum_form, left_op, right_op):
    return jnp.einsum(einsum_form, left_op.astype(jnp.float32), right_op.astype(jnp.float32))


def norm_forward(x_in, gain_f, shift_f):
    centered = x_in - jnp.mean(x_in, axis=-1, keepdims=True)
    inv_std = lax.rsqrt(jnp.mean(centered * centered, axis=-1, keepdims=True) + LN_EPS)
    x_hat = centered * inv_std
    return x_hat * gain_f + shift_f, x_hat, inv_std


def norm_backward(d_norm, x_hat, inv_std, gain_f):
    d_hat = d_norm * gain_f
    d_in = inv_std * (d_hat - jnp.mean(d_hat, axis=-1, keepdims=True) - x_hat * jnp.mean(d_hat * x_hat, axis=-1, keepdims=True))
    return d_in, jnp.sum(d_norm * x_hat, axis=(0, 1)), jnp.sum(d_norm, axis=(0, 1))


def gelu_slope(pre_act):
    return 0.5 * (1.0 + lax.erf(pre_act * INV_SQRT2)) + pre_act * jnp.exp(-0.5 * pre_act * pre_act) * INV_SQRT_2PI


def forward(full_w, patches, keep):
    n_img = patches.shape[0]
    d_model = full_w['w_out'].shape[0]
    n_heads, head_dim = full_w['w_qkv'].shape[2], full_w['w_qkv'].shape[3]
    logit_scale = head_dim ** -0.5
    as_f32 = {name: full_w[name].astype(jnp.float32) for name in VECTOR_NAMES}
    kept_rows = jnp.take_along_axis(patches, keep[:, :, None], axis=1)
    embed_rows = product('bkq,qw->bkw', kept_rows, full_w['w_patch']) + as_f32['b_patch'] + full_w['pos_table'][1 + keep].astype(jnp.float32)
    head_row = as_f32['cls_tok'] + full_w['pos_table'][0].astype(jnp.float32)
    x_zero = jnp.concatenate([jnp.broadcast_to(head_row, (n_img, 1, d_model)), embed_rows], axis=1)
    h_zero, hat_p, inv_p = norm_forward(x_zero, as_f32['lnp_g'], as_f32['lnp_b'])
    y_one, hat_1, inv_1 = norm_forward(h_zero, as_f32['ln1_g'], as_f32['ln1_b'])
    a_in = y_one.astype(jnp.bfloat16)
    qkv_all = (product('btw,wchd->btchd', a_in, full_w['w_qkv']) + as_f32['b_qkv'].reshape(3, n_heads, head_dim)).astype(jnp.bfloat16)
    q_heads, k_heads, v_heads = qkv_all[:, :, 0], qkv_all[:, :, 1], qkv_all[:, :, 2]
    attn_prob = jax.nn.softmax(product('bqhd,bkhd->bhqk', q_heads, k_heads) * logit_scale, axis=-1)
    prob_b = attn_prob.astype(jnp.bfloat16)
    context = product('bhqk,bkhd->bqhd', prob_b, v_heads).astype(jnp.bfloat16)
    h_mid = h_zero + product('bqhd,hdw->bqw', context, full_w['w_out'].reshape(n_heads, head_dim, d_model)) + as_f32['b_out']
    y_two, hat_2, inv_2 = norm_forward(h_mid, as_f32['ln2_g'], as_f32['ln2_b'])
    c_in = y_two.astype(jnp.bfloat16)
    pre_act = product('btw,wf->btf', c_in, full_w['w_fc']) + as_f32['b_fc']
    gelu_out = jax.nn.gelu(pre_act, approximate=False).astype(jnp.bfloat16)
    h_one = (h_mid + product('btf,fw->btw', gelu_out, full_w['w_proj']) + as_f32['b_proj']).astype(jnp.bfloat16)
    saved = dict(keep=keep, kept_rows=kept_rows, hat_p=hat_p, inv_p=inv_p, hat_1=hat_1, inv_1=inv_1, a_in=a_in, q_heads=q_heads, k_heads=k_heads, v_heads=v_heads, attn_prob=attn_prob, prob_b=prob_b, context=context, hat_2=hat_2, inv_2=inv_2, c_in=c_in, pre_act=pre_act, gelu_out=gelu_out)
    return h_one, saved


def backward(weights, saved, grad_h1):
    d_model = weights['w_out'].shape[0]
    n_heads, head_dim = weights['w_qkv'].shape[2], weights['w_qkv'].shape[3]
    logit_scale = head_dim ** -0.5
    w_out3 = weights['w_out'].reshape(n_heads, head_dim, d_model)
    d_h = grad_h1.astype(jnp.float32)
    g_w_proj = product('btf,btw->fw', saved['gelu_out'], grad_h1)
    d_pre = product('btw,fw->btf', grad_h1, weights['w_proj']) * gelu_slope(saved['pre_act'])
    d_pre_b = d_pre.astype(jnp.bfloat16)
    g_w_fc = product('btw,btf->wf', saved['c_in'], d_pre_b)
    d_c = product('btf,wf->btw', d_pre_b, weights['w_fc'])
    d_norm2, g_ln2_g, g_ln2_b = norm_backward(d_c, saved['hat_2'], saved['inv_2'], weights['ln2_g'].astype(jnp.float32))
    d_mid = d_norm2 + d_h
    d_mid_b = d_mid.astype(jnp.bfloat16)
    g_w_out = product('bqhd,bqw->hdw', saved['context'], d_mid_b).reshape(d_model, d_model)
    d_ctx = product('bqw,hdw->bqhd', d_mid_b, w_out3).astype(jnp.bfloat16)
    g_v = product('bhqk,bqhd->bkhd', saved['prob_b'], d_ctx)
    d_prob = product('bqhd,bkhd->bhqk', d_ctx, saved['v_heads'])
    attn_prob = saved['attn_prob']
    d_logit = (attn_prob * (d_prob - jnp.sum(attn_prob * d_prob, axis=-1, keepdims=True)) * logit_scale).astype(jnp.bfloat16)
    g_q = product('bhqk,bkhd->bqhd', d_logit, saved['k_heads'])
    g_k = product('bhqk,bqhd->bkhd', d_logit, saved['q_heads'])
    d_qkv = jnp.stack([g_q, g_k, g_v], axis=2)
    d_qkv_b = d_qkv.astype(jnp.bfloat16)
    g_w_qkv = product('btw,btchd->wchd', saved['a_in'], d_qkv_b)
    d_a = product('btchd,wchd->btw', d_qkv_b, weights['w_qkv'])
    d_norm1, g_ln1_g, g_ln1_b = norm_backward(d_a, saved['hat_1'], saved['inv_1'], weights['ln1_g'].astype(jnp.float32))
    d_zero = d_norm1 + d_mid
    d_x, g_lnp_g, g_lnp_b = norm_backward(d_zero, saved['hat_p'], saved['inv_p'], weights['lnp_g'].astype(jnp.float32))
    d_head = jnp.sum(d_x[:, 0], axis=0)
    d_emb = d_x[:, 1:]
    d_emb_b = d_emb.astype(jnp.bfloat16)
    pos_rest = jax.ops.segment_sum(d_emb_b.astype(jnp.float32).reshape(-1, d_model), saved['keep'].reshape(-1), num_segments=NUM_PATCHES)
    g_pos = jnp.concatenate([d_head[None], pos_rest], axis=0)
    return dict(w_patch=product('bkq,bkw->qw', saved['kept_rows'], d_emb_b), b_patch=jnp.sum(d_emb, axis=(0, 1)), pos_table=g_pos, cls_tok=d_head, lnp_g=g_lnp_g, lnp_b=g_lnp_b, ln1_g=g_ln1_g, ln1_b=g_ln1_b, w_qkv=g_w_qkv, b_qkv=jnp.sum(d_qkv, axis=(0, 1)).reshape(-1), w_out=g_w_out, b_out=jnp.sum(d_mid, axis=(0, 1)), ln2_g=g_ln2_g, ln2_b=g_ln2_b, w_fc=g_w_fc, b_fc=jnp.sum(d_pre, axis=(0, 1)), w_proj=g_w_proj, b_proj=jnp.sum(d_h, axis=(0, 1)))


def reference(patches, keep, w_patch, b_patch, pos_table, cls_tok, lnp_g, lnp_b, ln1_g, ln1_b, w_qkv, b_qkv, w_out, b_out, ln2_g, ln2_b, w_fc, b_fc, w_proj, b_proj, grad_h1):
    masters = (w_patch, b_patch, pos_table, cls_tok, lnp_g, lnp_b, ln1_g, ln1_b, w_qkv, b_qkv, w_out, b_out, ln2_g, ln2_b, w_fc, b_fc, w_proj, b_proj)
    full_w = {name: value.astype(jnp.bfloat16) for name, value in zip(PARAM_NAMES, masters)}
    n_blocks = BATCH_SIZE // BLOCK_IMAGES

    def split_blocks(array_in):
        return array_in.reshape((n_blocks, BLOCK_IMAGES) + array_in.shape[1:])

    def scan_step(running, block_in):
        h_one, saved = forward(full_w, block_in[0], block_in[1])
        grad_map = backward(full_w, saved, block_in[2])
        return {name: running[name] + grad_map[name] for name in PARAM_NAMES}, h_one

    zero_grads = {name: jnp.zeros(value.shape, jnp.float32) for name, value in zip(PARAM_NAMES, masters)}
    totals, h_blocks = lax.scan(scan_step, zero_grads, (split_blocks(patches), split_blocks(keep), split_blocks(grad_h1)))
    h_out = h_blocks.reshape(BATCH_SIZE, TOKENS, MODEL_WIDTH)
    return (h_out, totals['w_patch'], totals['b_patch'], totals['pos_table'], totals['cls_tok'], totals['lnp_g'], totals['lnp_b'], totals['ln1_g'], totals['ln1_b'], totals['w_qkv'], totals['b_qkv'], totals['w_out'], totals['b_out'], totals['ln2_g'], totals['ln2_b'], totals['w_fc'], totals['b_fc'], totals['w_proj'], totals['b_proj'])
```

```python
import functools

import jax
import jax.numpy as jnp
from jax import lax
from jax.experimental import pallas as pl
from jax.experimental.pallas import tpu as pltpu
from jax.sharding import PartitionSpec as P

AXIS = 'fsdp'
LN_EPS = 1e-5
INV_SQRT2 = 0.7071067811865476
INV_SQRT_2PI = 0.3989422804014327
PARAM_NAMES = ('w_patch', 'b_patch', 'pos_table', 'cls_tok', 'lnp_g', 'lnp_b', 'ln1_g', 'ln1_b', 'w_qkv', 'b_qkv', 'w_out', 'b_out', 'ln2_g', 'ln2_b', 'w_fc', 'b_fc', 'w_proj', 'b_proj')
VECTOR_NAMES = ('b_patch', 'cls_tok', 'lnp_g', 'lnp_b', 'ln1_g', 'ln1_b', 'b_out', 'ln2_g', 'ln2_b', 'b_proj', 'b_qkv', 'b_fc')
LAST_SPLIT = ('w_patch', 'pos_table')

BF = jnp.bfloat16
F32 = jnp.float32
X, Y, Z = 1, 2, 4
ORDERS = ((X, Y, Z), (Y, Z, X), (Z, X, Y))
PATCH_PAD = 896
VMEM = 60 * 1024 * 1024


def dot(a, b, ca, cb):
    return lax.dot_general(a, b, (((ca,), (cb,)), ((), ())), preferred_element_type=F32)


def swap(x, bit):
    return lax.ppermute(x, AXIS, [(i, i ^ bit) for i in range(16)])


def keep_order(bits):
    b0, b1, b2 = bits
    return (b1 | b2, b1, b2, 0)


def cost(flops, nbytes, trans=0):
    return pl.CostEstimate(flops=int(flops), bytes_accessed=int(nbytes), transcendentals=int(trans))


def fc_kernel(c_ref, w_ref, b_ref, g_ref, s_ref):
    u = dot(c_ref[...], w_ref[...], 1, 0) + b_ref[...]
    phi = 0.5 * (1.0 + lax.erf(u * INV_SQRT2))
    g_ref[...] = (u * phi).astype(BF)
    s_ref[...] = phi + u * jnp.exp(-0.5 * u * u) * INV_SQRT_2PI


def fc_gelu(c_in, w_fc, b_fc):
    m, k = c_in.shape
    n = w_fc.shape[1]
    tn = 256
    return pl.pallas_call(
        fc_kernel,
        grid=(n // tn,),
        in_specs=[pl.BlockSpec((m, k), lambda i: (0, 0)), pl.BlockSpec((k, tn), lambda i: (0, i)), pl.BlockSpec((1, tn), lambda i: (0, i))],
        out_specs=[pl.BlockSpec((m, tn), lambda i: (0, i)), pl.BlockSpec((m, tn), lambda i: (0, i))],
        out_shape=[jax.ShapeDtypeStruct((m, n), BF), jax.ShapeDtypeStruct((m, n), F32)],
        compiler_params=pltpu.CompilerParams(vmem_limit_bytes=VMEM),
        cost_estimate=cost(2 * m * n * k * 3, m * n * 6 + k * n * 2),
        name='fc_gelu',
    )(c_in, w_fc, b_fc)


def dpre_kernel(g_ref, w_ref, s_ref, d_ref, b_ref):
    d = dot(g_ref[...], w_ref[...], 1, 1) * s_ref[...]
    d_ref[...] = d.astype(BF)
    b_ref[...] = jnp.sum(d, axis=0, keepdims=True)


def d_pre(grad, w_proj, slope):
    m, k = grad.shape
    n = w_proj.shape[0]
    tn = 256
    return pl.pallas_call(
        dpre_kernel,
        grid=(n // tn,),
        in_specs=[pl.BlockSpec((m, k), lambda i: (0, 0)), pl.BlockSpec((tn, k), lambda i: (i, 0)), pl.BlockSpec((m, tn), lambda i: (0, i))],
        out_specs=[pl.BlockSpec((m, tn), lambda i: (0, i)), pl.BlockSpec((1, tn), lambda i: (0, i))],
        out_shape=[jax.ShapeDtypeStruct((m, n), BF), jax.ShapeDtypeStruct((1, n), F32)],
        compiler_params=pltpu.CompilerParams(vmem_limit_bytes=VMEM),
        cost_estimate=cost(2 * m * n * k * 1.5, m * n * 6 + k * n * 2),
        name='d_pre',
    )(grad, w_proj, slope)


def attn_masks(n_pat, n_img, i):
    t = n_pat + 2 * n_img
    r = lax.broadcasted_iota(jnp.int32, (t, t), 0)
    c = lax.broadcasted_iota(jnp.int32, (t, t), 1)
    ok_r = (r < n_pat) | (r == n_pat + i)
    ok_c = (c < n_pat) | (c == n_pat + i)
    return ok_r, ok_c


def take_ext(ref, n_pat, n_img, start, lead=None):
    if lead is None:
        body = ref[pl.ds(start, n_pat), :]
        tail = ref[pl.ds(n_pat * n_img, n_img), :]
    else:
        body = ref[lead, pl.ds(start, n_pat), :]
        tail = ref[lead, pl.ds(n_pat * n_img, n_img), :]
    tail = tail.astype(F32)
    tail = jnp.concatenate([tail, jnp.zeros_like(tail)], axis=0).astype(BF)
    return jnp.concatenate([body, tail], axis=0)


def lane_half(x, h, hd):
    lane = lax.broadcasted_iota(jnp.int32, x.shape, 1)
    return jnp.where((lane >= h * hd) & (lane < (h + 1) * hd), x, jnp.zeros_like(x))


def softmax_ext(q, k, ok_r, ok_c, scale):
    s = jnp.where(ok_c, dot(q, k, 1, 1) * scale, -jnp.inf)
    e = jnp.exp(s - jnp.max(s, axis=1, keepdims=True))
    inv = 1.0 / jnp.sum(e, axis=1, keepdims=True)
    return jnp.where(ok_r, e * inv, 0.0)


def attn_fwd_kernel(n_img, n_pat, hd, scale, q_ref, k_ref, v_ref, o_ref, tail_ref):
    tail_ref[...] = jnp.zeros_like(tail_ref)

    def body(i, _):
        start = pl.multiple_of(i * n_pat, n_pat)
        q = take_ext(q_ref, n_pat, n_img, start)
        k = take_ext(k_ref, n_pat, n_img, start)
        v = take_ext(v_ref, n_pat, n_img, start)
        ok_r, ok_c = attn_masks(n_pat, n_img, i)
        o = None
        for h in range(2):
            p = softmax_ext(lane_half(q, h, hd), k, ok_r, ok_c, scale)
            oh = dot(p.astype(BF), lane_half(v, h, hd), 1, 0)
            o = oh if o is None else o + oh
        o_ref[pl.ds(start, n_pat), :] = o[:n_pat].astype(BF)
        tail_ref[...] += o[n_pat:n_pat + n_img]
        return 0

    lax.fori_loop(0, n_img, body, 0)
    o_ref[pl.ds(n_pat * n_img, n_img), :] = tail_ref[...].astype(BF)


def attn_fwd(qkv, n_img, n_pat, n_heads, hd):
    m = qkv.shape[0]
    n = n_heads * hd
    blk = 2 * hd
    nb = n // blk
    return pl.pallas_call(
        functools.partial(attn_fwd_kernel, n_img, n_pat, hd, hd ** -0.5),
        grid=(nb,),
        in_specs=[pl.BlockSpec((m, blk), lambda h: (0, h)), pl.BlockSpec((m, blk), lambda h: (0, nb + h)), pl.BlockSpec((m, blk), lambda h: (0, 2 * nb + h))],
        out_specs=pl.BlockSpec((m, blk), lambda h: (0, h)),
        out_shape=jax.ShapeDtypeStruct((m, n), BF),
        scratch_shapes=[pltpu.VMEM((n_img, blk), F32)],
        compiler_params=pltpu.CompilerParams(vmem_limit_bytes=VMEM),
        cost_estimate=cost(2 * m * n * 256 * 20, m * n * 8),
        name='attn_fwd',
    )(qkv, qkv, qkv)


def attn_bwd_kernel(n_img, n_pat, hd, scale, q_ref, k_ref, v_ref, do_ref, d_ref, b_ref, tail_ref):
    tail_ref[...] = jnp.zeros_like(tail_ref)
    b_ref[...] = jnp.zeros_like(b_ref)

    def body(i, _):
        start = pl.multiple_of(i * n_pat, n_pat)
        q = take_ext(q_ref, n_pat, n_img, start)
        k = take_ext(k_ref, n_pat, n_img, start)
        v = take_ext(v_ref, n_pat, n_img, start)
        do = take_ext(do_ref, n_pat, n_img, start)
        ok_r, ok_c = attn_masks(n_pat, n_img, i)
        acc = [None, None, None]
        for h in range(2):
            qh, kh, doh = lane_half(q, h, hd), lane_half(k, h, hd), lane_half(do, h, hd)
            p = softmax_ext(qh, k, ok_r, ok_c, scale)
            dp = dot(doh, v, 1, 1)
            dl = (p * (dp - jnp.sum(p * dp, axis=1, keepdims=True)) * scale).astype(BF)
            pb = p.astype(BF)
            parts = (dot(dl, kh, 1, 0), dot(dl, qh, 0, 0), dot(pb, doh, 0, 0))
            acc = [x if a is None else a + x for a, x in zip(acc, parts)]
        for s in range(3):
            d_ref[s, pl.ds(start, n_pat), :] = acc[s][:n_pat].astype(BF)
            tail_ref[s] += acc[s][n_pat:n_pat + n_img]
            b_ref[0, pl.ds(s, 1), :] += jnp.sum(acc[s][:n_pat], axis=0, keepdims=True)
        return 0

    lax.fori_loop(0, n_img, body, 0)
    for s in range(3):
        t = tail_ref[s]
        d_ref[s, pl.ds(n_pat * n_img, n_img), :] = t.astype(BF)
        b_ref[0, pl.ds(s, 1), :] += jnp.sum(t, axis=0, keepdims=True)


def attn_bwd(qkv, d_ctx, n_img, n_pat, n_heads, hd):
    m = qkv.shape[0]
    n = n_heads * hd
    blk = 2 * hd
    nb = n // blk
    d3, b3 = pl.pallas_call(
        functools.partial(attn_bwd_kernel, n_img, n_pat, hd, hd ** -0.5),
        grid=(nb,),
        in_specs=[pl.BlockSpec((m, blk), lambda h: (0, h)), pl.BlockSpec((m, blk), lambda h: (0, nb + h)), pl.BlockSpec((m, blk), lambda h: (0, 2 * nb + h)), pl.BlockSpec((m, blk), lambda h: (0, h))],
        out_specs=[pl.BlockSpec((3, m, blk), lambda h: (0, 0, h)), pl.BlockSpec((1, 8, blk), lambda h: (h, 0, 0))],
        out_shape=[jax.ShapeDtypeStruct((3, m, n), BF), jax.ShapeDtypeStruct((nb, 8, blk), F32)],
        scratch_shapes=[pltpu.VMEM((3, n_img, blk), F32)],
        compiler_params=pltpu.CompilerParams(vmem_limit_bytes=VMEM),
        cost_estimate=cost(2 * m * n * 256 * 40, m * n * 14),
        name='attn_bwd',
    )(qkv, qkv, qkv, d_ctx)
    return d3, b3[:, :3].transpose(1, 0, 2).reshape(3, n)


def dw_kernel(order, bit0, rows, lo_ref, lr_ref, ro_ref, rr_ref, s_ref, k_ref):
    ro = ro_ref[0] if len(ro_ref.shape) == 3 else ro_ref[...]
    rr = rr_ref[0] if len(rr_ref.shape) == 3 else rr_ref[...]
    acc = dot(lo_ref[...], ro, 1, 0) + dot(lr_ref[...], rr, 1, 0)
    for pos, j in enumerate(order):
        k_ref[pos * rows:(pos + 1) * rows, :] = acc[j * rows:(j + 1) * rows]
        j1 = j ^ bit0
        s_ref[pos * rows:(pos + 1) * rows, :] = acc[j1 * rows:(j1 + 1) * rows]


def dw(lt_own, lt_rcv, r_own, r_rcv, bits, off, ncols, tn, lead=None):
    mrows, k = lt_own.shape
    if lead is None:
        r_spec = pl.BlockSpec((k, tn), lambda i: (0, off // tn + i))
    else:
        r_spec = pl.BlockSpec((1, k, tn), lambda i: (lead, 0, off // tn + i))
    l_spec = pl.BlockSpec((mrows, k), lambda i: (0, 0))
    o_spec = pl.BlockSpec((mrows // 2, tn), lambda i: (0, i))
    o_shape = jax.ShapeDtypeStruct((mrows // 2, ncols), F32)
    return pl.pallas_call(
        functools.partial(dw_kernel, keep_order(bits), bits[0], mrows // 8),
        grid=(ncols // tn,),
        in_specs=[l_spec, l_spec, r_spec, r_spec],
        out_specs=[o_spec, o_spec],
        out_shape=[o_shape, o_shape],
        compiler_params=pltpu.CompilerParams(vmem_limit_bytes=VMEM),
        cost_estimate=cost(4 * mrows * ncols * k * 1.5, mrows * (4 * k + 4 * ncols) + 4 * k * ncols),
        name='dw',
    )(lt_own, lt_rcv, r_own, r_rcv)


def dwp_kernel(idx_ref, lo_ref, lr_ref, ro_ref, rr_ref, s_ref, k_ref):
    acc = dot(lo_ref[...], ro_ref[...], 0, 0) + dot(lr_ref[...], rr_ref[...], 0, 0)
    half = pl.program_id(0)

    @pl.when(half == 0)
    def _():
        s_ref[...] = acc

    @pl.when(half == 1)
    def _():
        k_ref[...] = acc


def dw_proj(gelu, gelu_rcv, r_own, r_rcv, bits, off, ncols, chip, core):
    m = gelu.shape[0]
    rows = gelu.shape[1] // 16
    order = keep_order(bits)
    js = jnp.array([j ^ bits[0] for j in order] + list(order), jnp.int32) ^ chip
    idx = jnp.stack([js, js * 2 + core])
    o_spec_s = pl.BlockSpec((rows, ncols), lambda h, i, t: (jnp.where(h == 0, i, 3), 0))
    o_spec_k = pl.BlockSpec((rows, ncols), lambda h, i, t: (jnp.where(h == 0, 0, i), 0))
    o_shape = jax.ShapeDtypeStruct((4 * rows, ncols), F32)
    r_spec = pl.BlockSpec((m, ncols), lambda h, i, t: (0, 0))
    return pl.pallas_call(
        dwp_kernel,
        grid_spec=pltpu.PrefetchScalarGridSpec(
            num_scalar_prefetch=1,
            grid=(2, 4),
            in_specs=[pl.BlockSpec((m, rows), lambda h, i, t: (0, t[1, h * 4 + i])), pl.BlockSpec((m, rows), lambda h, i, t: (0, t[0, h * 4 + i])), r_spec, r_spec],
            out_specs=[o_spec_s, o_spec_k],
        ),
        out_shape=[o_shape, o_shape],
        compiler_params=pltpu.CompilerParams(vmem_limit_bytes=VMEM),
        cost_estimate=cost(4 * 8 * rows * ncols * m * 1.5, m * rows * 32 + 4 * m * ncols + 32 * rows * ncols),
        name='dw_proj',
    )(idx, gelu, gelu_rcv, r_own[:, off:off + ncols], r_rcv[:, off:off + ncols])


def reduce_part(send, keep, bits):
    for stage, bit in enumerate(bits):
        got = swap(send, 2 * bit)
        if stage == 2:
            return keep + got
        half = keep.shape[0] // 2
        send = keep[:half] + got[:half]
        keep = keep[half:] + got[half:]


def norm_forward(x_in, gain_f, shift_f):
    centered = x_in - jnp.mean(x_in, axis=-1, keepdims=True)
    inv_std = lax.rsqrt(jnp.mean(centered * centered, axis=-1, keepdims=True) + LN_EPS)
    x_hat = centered * inv_std
    return x_hat * gain_f + shift_f, x_hat, inv_std


def norm_backward(d_norm, x_hat, inv_std, gain_f):
    d_hat = d_norm * gain_f
    d_in = inv_std * (d_hat - jnp.mean(d_hat, axis=-1, keepdims=True) - x_hat * jnp.mean(d_hat * x_hat, axis=-1, keepdims=True))
    return d_in, jnp.sum(d_norm * x_hat, axis=0), jnp.sum(d_norm, axis=0)


def solution(mesh):
    def spec_of(name):
        return P(None, AXIS) if name in LAST_SPLIT else P(AXIS)

    def local_step(patches, keep, *rest):
        shard = dict(zip(PARAM_NAMES, rest[:-1]))
        grad_h1 = rest[-1]
        n_img, n_patch, n_pix = patches.shape
        n_keep = keep.shape[1]
        d_model = shard['w_out'].shape[1]
        n_heads, hd = shard['w_qkv'].shape[2], shard['w_qkv'].shape[3]
        me = lax.axis_index(AXIS)
        core, chip = me % 2, me // 2
        rows = d_model // 16
        n_tok = n_img * n_keep

        def gather(x):
            return lax.all_gather(x.astype(BF), AXIS, axis=0, tiled=True)

        vec_cols = [shard[name].astype(BF).reshape(-1, rows) for name in VECTOR_NAMES]
        vec_local = jnp.concatenate(vec_cols, axis=0)
        n_vec = vec_local.shape[0]
        small = jnp.concatenate([shard['w_patch'].T.astype(BF), shard['pos_table'].T.astype(BF), vec_local.T], axis=1)
        used = small.shape[1]
        small = jnp.pad(small, ((0, 0), (0, PATCH_PAD - used)))
        small_all = gather(small)
        w_qkv = gather(shard['w_qkv'].astype(BF).reshape(rows, -1))
        w_out = gather(shard['w_out'])
        w_fc = gather(shard['w_fc'])
        w_proj = gather(shard['w_proj'])

        n_emb = n_pix + n_patch + 1
        vec_all = small_all[:, n_emb:n_emb + n_vec].T.astype(F32)
        vec = {name: vec_all[i] for i, name in enumerate(VECTOR_NAMES[:10])}
        b_qkv = vec_all[10:13].reshape(3, 16, rows).transpose(1, 0, 2).reshape(1, -1)
        b_fc = vec_all[13:17].reshape(4, 16, rows).transpose(1, 0, 2).reshape(1, -1)

        onehot = (keep[:, :, None] == lax.broadcasted_iota(jnp.int32, (1, 1, n_patch), 2)).astype(BF)
        kept = jnp.einsum('bkp,bpq->bkq', onehot, patches, preferred_element_type=F32).astype(BF)
        emb_in = jnp.concatenate([kept, jnp.zeros((n_img, n_keep, 1), BF), onehot, jnp.zeros((n_img, n_keep, PATCH_PAD - n_emb), BF)], axis=2).reshape(n_tok, PATCH_PAD)
        emb_rcv = swap(emb_in, 1)
        embed = dot(emb_in, small_all, 1, 1) + vec['b_patch']
        head_row = vec['cls_tok'] + small_all[:, n_pix].astype(F32)
        x_zero = jnp.concatenate([embed, jnp.broadcast_to(head_row, (n_img, d_model))], axis=0)
        h_zero, hat_p, inv_p = norm_forward(x_zero, vec['lnp_g'], vec['lnp_b'])
        y_one, hat_1, inv_1 = norm_forward(h_zero, vec['ln1_g'], vec['ln1_b'])
        a_in = y_one.astype(BF)
        qkv = (dot(a_in, w_qkv, 1, 0) + b_qkv).astype(BF)
        ctx = attn_fwd(qkv, n_img, n_keep, n_heads, hd)
        h_mid = h_zero + dot(ctx, w_out, 1, 0) + vec['b_out']
        y_two, hat_2, inv_2 = norm_forward(h_mid, vec['ln2_g'], vec['ln2_b'])
        c_in = y_two.astype(BF)
        gelu, slope = fc_gelu(c_in, w_fc, b_fc)
        h_flat = (h_mid + dot(gelu, w_proj, 1, 0) + vec['b_proj']).astype(BF)
        h_one = jnp.concatenate([h_flat[n_tok:, None], h_flat[:n_tok].reshape(n_img, n_keep, d_model)], axis=1)

        grad = jnp.concatenate([grad_h1[:, 1:].reshape(n_tok, d_model), grad_h1[:, 0]], axis=0)
        grad_f = grad.astype(F32)
        grad_rcv = swap(grad, 1)

        col = lax.broadcasted_iota(jnp.int32, (8 * rows, d_model), 1)
        row = lax.broadcasted_iota(jnp.int32, (8 * rows, d_model), 0)
        base = (((row // rows) ^ chip) * 2) * rows + row % rows
        sel_own = (col == base + core * rows).astype(BF)
        sel_other = (col == base + (1 - core) * rows).astype(BF)

        def picked(x):
            own = dot(sel_own, x, 1, 1).astype(BF)
            other = dot(sel_other, x, 1, 1).astype(BF)
            return own, swap(other, 1)

        blk = gelu.shape[1] // 16
        other = lax.dynamic_index_in_dim(gelu.reshape(-1, 8, 2, blk), 1 - core, 2, keepdims=False).reshape(gelu.shape[0], -1)
        gelu_rcv = swap(other, 1)
        g_proj = []
        off = 0
        for ncols, bits in zip((256, 384, 384), ORDERS):
            s, k = dw_proj(gelu, gelu_rcv, grad, grad_rcv, bits, off, ncols, chip, core)
            g_proj.append(reduce_part(s, k, bits))
            off += ncols

        d_pre_b, g_bfc = d_pre(grad, w_proj, slope)
        dpre_rcv = swap(d_pre_b, 1)
        c_own, c_rcv = picked(c_in)
        g_fc = []
        off = 0
        for ncols, bits in zip((1536, 1280, 1280), ORDERS):
            s, k = dw(c_own, c_rcv, d_pre_b, dpre_rcv, bits, off, ncols, 256)
            g_fc.append(reduce_part(s, k, bits))
            off += ncols
        d_c = dot(d_pre_b, w_fc, 1, 1)
        d_n2, g_ln2_g, g_ln2_b = norm_backward(d_c, hat_2, inv_2, vec['ln2_g'])
        d_mid = d_n2 + grad_f
        d_mid_b = d_mid.astype(BF)
        dmid_rcv = swap(d_mid_b, 1)
        o_own, o_rcv = picked(ctx)
        g_out = []
        off = 0
        for ncols, bits in zip((512, 256, 256), ORDERS):
            s, k = dw(o_own, o_rcv, d_mid_b, dmid_rcv, bits, off, ncols, 256)
            g_out.append(reduce_part(s, k, bits))
            off += ncols
        d_ctx = dot(d_mid_b, w_out, 1, 1).astype(BF)
        d3, g_bqkv = attn_bwd(qkv, d_ctx, n_img, n_keep, n_heads, hd)
        d3_rcv = swap(d3, 1)
        a_own, a_rcv = picked(a_in)
        g_qkv = []
        for lead, bits in enumerate(ORDERS):
            s, k = dw(a_own, a_rcv, d3, d3_rcv, bits, 0, d_model, 256, lead=lead)
            g_qkv.append(reduce_part(s, k, bits))
        w3 = w_qkv.reshape(d_model, 3, d_model)
        d_a = dot(d3[0], w3[:, 0], 1, 1) + dot(d3[1], w3[:, 1], 1, 1) + dot(d3[2], w3[:, 2], 1, 1)
        d_n1, g_ln1_g, g_ln1_b = norm_backward(d_a, hat_1, inv_1, vec['ln1_g'])
        d_zero = d_n1 + d_mid
        d_x, g_lnp_g, g_lnp_b = norm_backward(d_zero, hat_p, inv_p, vec['lnp_g'])
        d_emb = d_x[:n_tok]
        d_emb_b = d_emb.astype(BF)
        e_own, e_rcv = picked(d_emb_b)
        g_emb = []
        off = 0
        for ncols, bits in zip((256, 384, 256), ORDERS):
            s, k = dw(e_own, e_rcv, emb_in, emb_rcv, bits, off, ncols, 128)
            g_emb.append(reduce_part(s, k, bits))
            off += ncols

        g_cls = jnp.sum(d_x[n_tok:], axis=0)
        sums = dict(b_patch=jnp.sum(d_emb, axis=0), cls_tok=g_cls, lnp_g=g_lnp_g, lnp_b=g_lnp_b, ln1_g=g_ln1_g, ln1_b=g_ln1_b, b_out=jnp.sum(d_mid, axis=0), ln2_g=g_ln2_g, ln2_b=g_ln2_b, b_proj=jnp.sum(grad_f, axis=0), b_qkv=g_bqkv.reshape(-1), b_fc=g_bfc.reshape(-1))
        stack = jnp.concatenate([sums[name].reshape(16, -1) for name in VECTOR_NAMES], axis=1)
        part = stack.reshape(2, 2, 2, 2, -1)
        for axis, bit in ((3, 1), (2, 2), (1, 4), (0, 8)):
            b = (me // bit) % 2
            got = swap(lax.dynamic_index_in_dim(part, 1 - b, axis, keepdims=False), bit)
            part = lax.dynamic_index_in_dim(part, b, axis, keepdims=False) + got

        grads = {}
        off = 0
        for name in VECTOR_NAMES:
            n = shard[name].shape[0]
            grads[name] = part[off:off + n]
            off += n
        emb = jnp.concatenate(g_emb, axis=1).T
        grads['w_patch'] = emb[:n_pix]
        grads['pos_table'] = jnp.concatenate([grads['cls_tok'][None], emb[n_pix + 1:n_emb]], axis=0)
        grads['w_qkv'] = jnp.stack(g_qkv, axis=1).reshape(shard['w_qkv'].shape)
        grads['w_out'] = jnp.concatenate(g_out, axis=1)
        grads['w_fc'] = jnp.concatenate(g_fc, axis=1)
        grads['w_proj'] = jnp.concatenate(g_proj, axis=1)
        return (h_one,) + tuple(grads[name] for name in PARAM_NAMES)

    batch_spec = P(AXIS)
    param_specs = tuple(spec_of(name) for name in PARAM_NAMES)
    return jax.shard_map(local_step, mesh=mesh, in_specs=(batch_spec, batch_spec) + param_specs + (batch_spec,), out_specs=(batch_spec,) + param_specs, check_vma=False)
```
